128 devices in a mesh: group: 4 (over z_lo, core), fsdp: 32 (over y, x, z_hi).
Axes of the slice: x: 4, y: 4, z: 4 (z_hi: 2, z_lo: 2; z = z_hi * 2 + z_lo), core: 2. Of those that a mesh axis runs over, the one named last changes fastest.
Arguments:
- tokens: bfloat16 [65536, 3072], P(('group', 'fsdp')), may hold values from -6 to 6
- student: float32 [4, 3072, 6144], P('group', 'fsdp'), may hold values from -6 to 6
- teacher: float32 [3072, 6144], P('fsdp', 'group'), may hold values from -6 to 6
- norm_gain: float32 [3072], replicated, may hold values from 0.5 to 1.5
- query_gain: float32 [128], replicated, may hold values from 0.5 to 1.5
- key_gain: float32 [128], replicated, may hold values from 0.5 to 1.5
Outputs:
- teacher_new: float32 [3072, 6144], P('fsdp', 'group')
- student_new: float32 [3072, 6144], P('fsdp', 'group')
- query: bfloat16 [65536, 3072], P(('group', 'fsdp'))
- key: bfloat16 [65536, 3072], P(('group', 'fsdp'))
The draws below stay inside these ranges and needn't reach their ends.
All inputs are finite; a program needn't handle non-finite values.
Results may differ from the reference program's by a relative error of at most 0.0058.
Values may be sent and summed in bfloat16 or wider, within the bound.
No kernel may reach another device: no remote copies, remote signals or barrier semaphores. Data moves between devices by JAX's collectives and lax.ppermute only.
A program may use at most 192 MiB of HBM per device.

```python
import jax
import jax.numpy as jnp
from jax import lax

D = 3072
HEAD = 128
TOK_DEV = 512
GROUPS = 4
TOKENS = 65536
N_GROUP = 4
N_FSDP = 32


def raised(result, rng, source, target, blocks, factor):
    owner, partner = [(jnp.arange(result.shape[axis_at]) // (result.shape[axis_at] // blocks)).reshape([-1 if axis == axis_at else 1 for axis in range(result.ndim)]) for axis_at in (source, target)]
    chosen = jax.random.permutation(rng, blocks)[partner]
    strong = (owner == chosen) | (owner == (partner + blocks // 2) % blocks)
    return jnp.where(strong, factor * result, result)


def shard_levels(own_key, dims, shards, least, top_value):
    def one(position, blocks):
        draws = jax.random.uniform(jax.random.fold_in(jax.random.fold_in(own_key, 6), position), (blocks,), jnp.float32, least / len(shards), top_value / len(shards))
        return jnp.repeat(jnp.exp(draws), dims[position] // blocks).reshape((-1,) + (1,) * (len(dims) - position - 1))

    factor_of = one(*shards[0])
    for cut in shards[1:]:
        factor_of = factor_of * one(*cut)
    return factor_of


def noise(stream_key, extent, scale, most, shards=(), dtype=jnp.bfloat16):
    values = jax.random.normal(stream_key, extent, jnp.float32) * scale
    if len(shards) > 0:
        values = shard_levels(stream_key, extent, shards, -0.22, 0.18) * values
    return jnp.clip(values, min=-most, max=most).astype(dtype)


def heavy_noise(stream_key, shape, scale, bound, pieces, heavy, held_as=jnp.bfloat16):
    entries = scale * jax.random.normal(stream_key, shape, jnp.float32)
    if pieces:
        entries = entries * shard_levels(stream_key, shape, pieces, -0.22, 0.18)
    return jnp.clip(raised(entries, jax.random.fold_in(stream_key, 3), *heavy), -bound, bound).astype(held_as)


def setup_inputs(seed: int = 0) -> dict:
    key_list = jax.random.split(jax.random.key(seed), 7)
    tokens = noise(key_list[0], (TOKENS, D), 1.0, 6.0, ((0, 128),))
    student = heavy_noise(key_list[1], (GROUPS, D, 2 * D), 1.0, 6.0, ((0, 4), (1, 32)), (0, 2, 4, 2.0), jnp.float32)
    teacher = noise(key_list[2], (D, 2 * D), 1.0, 6.0, ((0, 32), (1, 4)), jnp.float32)
    norm_gain = jnp.clip(1.0 + 0.1 * jax.random.normal(key_list[3], (D,), jnp.float32), 0.5, 1.5)
    query_gain = jnp.clip(1.0 + 0.1 * jax.random.normal(key_list[4], (HEAD,), jnp.float32), 0.5, 1.5)
    key_gain = jnp.clip(1.0 + 0.1 * jax.random.normal(key_list[5], (HEAD,), jnp.float32), 0.5, 1.5)
    return dict(tokens=tokens, student=student, teacher=teacher, norm_gain=norm_gain, query_gain=query_gain, key_gain=key_gain)


ema_decay = 0.99

def head_norm(values, gain):
    shaped = values.reshape(values.shape[0], D // HEAD, HEAD)
    scaled = shaped * lax.rsqrt(lax.optimization_barrier(jnp.mean(shaped * shaped, axis=-1, keepdims=True)) + 1e-06) * gain
    return scaled.reshape(values.shape[0], D).astype(jnp.bfloat16)

def reference(tokens, student, teacher, norm_gain, query_gain, key_gain):
    student_new = lax.optimization_barrier(jnp.sum(student, axis=0)) / N_GROUP
    teacher_new = ema_decay * teacher + (1.0 - ema_decay) * student_new
    copied = student_new.astype(jnp.bfloat16)
    blocks = tokens.reshape(N_GROUP * N_FSDP, TOK_DEV, D)

    def one_block(block):
        wide = block.astype(jnp.float32)
        normed = (wide * lax.rsqrt(lax.optimization_barrier(jnp.mean(wide * wide, axis=-1, keepdims=True)) + 1e-06) * norm_gain).astype(jnp.bfloat16)
        projected = jnp.dot(normed, copied, preferred_element_type=jnp.float32) * D ** (-0.5)
        return (head_norm(projected[:, :D], query_gain), head_norm(projected[:, D:], key_gain))
    query, key = lax.map(one_block, blocks)
    return (teacher_new, student_new, query.reshape(TOKENS, D), key.reshape(TOKENS, D))
```

```python
import jax
import jax.numpy as jnp
import numpy as np
from jax import lax
from jax.experimental import pallas as pl
from jax.experimental.pallas import tpu as pltpu
from jax.sharding import Mesh
from jax.sharding import PartitionSpec as P

HEAD = 128
EMA = 0.99
COLORS = 3
CHUNKS = 2
FIRST, SECOND = (1, 3), (3, 1)
ORDER = ((0, 1, 3, 2), (0, 3, 1, 2))
DIMS = (("x", "y", "z"), ("y", "z", "x"), ("z", "x", "y"))


def z_place(zlo, zhi):
    return 2 * zhi + zlo


def exchange(x, dim, masks):
    if dim == "z":
        axes = ("zlo", "core", "zhi")
        pairs = []
        for zlo in range(2):
            for core in range(2):
                for zhi in range(2):
                    z = z_place(zlo, zhi) ^ masks[core]
                    pairs.append(((zlo * 2 + core) * 2 + zhi, ((z % 2) * 2 + core) * 2 + z // 2))
    else:
        axes = ("core", dim)
        pairs = [(core * 4 + i, core * 4 + (i ^ masks[core])) for core in range(2) for i in range(4)]
    return lax.ppermute(x, axes, pairs)


def destinations():
    core = lax.axis_index("core")
    order = jnp.where(core == 0, jnp.array(ORDER[0], jnp.int32), jnp.array(ORDER[1], jnp.int32))
    own = {
        "x": lax.axis_index("x"),
        "y": lax.axis_index("y"),
        "z": z_place(lax.axis_index("zlo"), lax.axis_index("zhi")),
    }
    tables = []
    for dims in DIMS:
        shapes = dict(zip(dims, ((1, 1, 4), (1, 4, 1), (4, 1, 1))))
        at = {d: (own[d] ^ order).reshape(shapes[d]) for d in dims}
        row = (at["z"] % 2) * 32 + (at["y"] * 4 + at["x"]) * 2 + at["z"] // 2
        tables.append(row.reshape(64))
    return jnp.concatenate(tables).astype(jnp.int32)


def project_body(chunk, n, *refs):
    n_in = 4 + 4 * COLORS + (2 if chunk else 0)
    dest, core, tokens, gains = refs[0], refs[1], refs[2], refs[3]
    units = refs[4 : 4 + 4 * COLORS]
    q_out, k_out, send_out, held, sem = refs[n_in:]
    color = pl.program_id(0)
    rows = units[0].shape[1]

    def fetch(k):
        for u in range(4):
            src = units[4 * k + u]

            def one(pos, _):
                row = pl.multiple_of(dest[(4 * k + u) * 16 + pos] * rows, 16)
                pltpu.make_async_copy(src.at[pos], held.at[k % 2, pl.ds(row, rows)], sem.at[k % 2]).start()
                return _

            lax.fori_loop(0, 16, one, 0)

    @pl.when(color == 0)
    def _():
        fetch(0)

    for k in range(COLORS - 1):

        @pl.when(color == k)
        def _():
            fetch(k + 1)

    slot = color % 2
    pltpu.make_async_copy(held.at[slot], held.at[slot], sem.at[slot]).wait()
    width = tokens.shape[1]
    scale = width ** (-0.5)
    half = tokens.shape[0] // 2
    tile = 256
    for i, out in enumerate((q_out, k_out)):
        w = held[slot, i * width : (i + 1) * width, :]
        gain = gains[i : i + 1, :]
        for m in range(0, 2 * half, tile):
            y = jnp.dot(tokens[m : m + tile, :], w, preferred_element_type=jnp.float32) * scale
            parts = []
            for h in range(0, n, HEAD):
                v = y[:, h : h + HEAD]
                parts.append(v * lax.rsqrt(jnp.mean(v * v, axis=-1, keepdims=True) + 1e-06) * gain)
            done = jnp.concatenate(parts, axis=1).astype(jnp.bfloat16)
            if m < half:
                out[m : m + tile, :] = done
            else:
                send_out[i, m - half : m - half + tile, :] = done


def project(chunk, dest, core, tokens, gains, units, held_outputs, n):
    half = tokens.shape[0] // 2
    width = tokens.shape[1]
    col = lambda i, dest, core: (0, core[0] * COLORS * CHUNKS + i * CHUNKS + chunk)
    any_spec = pl.BlockSpec(memory_space=pl.ANY)
    operands = [tokens, gains, *units]
    specs = [
        pl.BlockSpec(tokens.shape, lambda i, *_: (0, 0)),
        pl.BlockSpec(gains.shape, lambda i, *_: (0, 0)),
    ] + [any_spec] * len(units)
    aliases = {}
    if held_outputs:
        aliases = {2 + len(operands): 0, 3 + len(operands): 1}
        operands += list(held_outputs)
        specs += [any_spec] * 2
    big = jax.ShapeDtypeStruct((half, width), jnp.bfloat16)
    return pl.pallas_call(
        lambda *refs: project_body(chunk, n, *refs),
        grid_spec=pltpu.PrefetchScalarGridSpec(
            num_scalar_prefetch=2,
            grid=(COLORS,),
            in_specs=specs,
            out_specs=[
                pl.BlockSpec((half, n), col),
                pl.BlockSpec((half, n), col),
                pl.BlockSpec((2, half, n), lambda i, *_: (0, 0, i)),
            ],
            scratch_shapes=[
                pltpu.VMEM((2, 2 * width, n), jnp.bfloat16),
                pltpu.SemaphoreType.DMA((2,)),
            ],
        ),
        out_shape=[big, big, jax.ShapeDtypeStruct((2, half, COLORS * n), jnp.bfloat16)],
        input_output_aliases=aliases,
        compiler_params=pltpu.CompilerParams(dimension_semantics=("arbitrary",), vmem_limit_bytes=50 * 2**20),
        cost_estimate=pl.CostEstimate(
            flops=2 * 2 * half * width * 2 * n * COLORS,
            bytes_accessed=2 * width * (2 * half + 2 * n * COLORS),
            transcendentals=0,
        ),
        name=f"project_{chunk}",
    )(dest, core, *operands)


def place_body(core, got, q_in, k_in, q_out, k_out):
    q_out[...] = got[0]
    k_out[...] = got[1]


def place(chunk, core, got, query, key_out, n):
    half = query.shape[0]
    col = lambda i, core: (0, (1 - core[0]) * COLORS * CHUNKS + i * CHUNKS + chunk)
    any_spec = pl.BlockSpec(memory_space=pl.ANY)
    return pl.pallas_call(
        place_body,
        grid_spec=pltpu.PrefetchScalarGridSpec(
            num_scalar_prefetch=1,
            grid=(COLORS,),
            in_specs=[pl.BlockSpec((2, half, n), lambda i, core: (0, 0, i)), any_spec, any_spec],
            out_specs=[pl.BlockSpec((half, n), col), pl.BlockSpec((half, n), col)],
        ),
        out_shape=[jax.ShapeDtypeStruct(query.shape, query.dtype)] * 2,
        input_output_aliases={2: 0, 3: 1},
        cost_estimate=pl.CostEstimate(flops=1000000000, bytes_accessed=4 * got.size, transcendentals=0),
        name=f"place_{chunk}",
    )(core, got, query, key_out)


def shards(tokens, student, teacher, norm_gain, query_gain, key_gain):
    width = tokens.shape[1]
    block = teacher.shape[1]
    core = lax.axis_index("core")
    zlo = lax.axis_index("zlo")
    swap = [(0, 1), (1, 0)]

    local = student[0]
    blocks = lambda c: jnp.stack([lax.dynamic_slice_in_dim(local, (2 * j + c) * block, block, 1) for j in range(2)])
    pair = blocks(core) + lax.ppermute(blocks(1 - core), "core", swap)
    n_color = block // COLORS
    keep = jnp.where(zlo == 0, pair[0], pair[1])
    give = jnp.where(zlo == 0, pair[1], pair[0])
    owned, copied = [], []
    for k in range(COLORS):
        cols = slice(k * n_color, (k + 1) * n_color)
        owned.append((keep[:, cols] + lax.ppermute(give[:, cols], "zlo", swap)) / 4)
        copied.append(owned[-1].astype(jnp.bfloat16)[None])
    student_new = jnp.concatenate(owned, axis=1)
    teacher_new = EMA * teacher + (1.0 - EMA) * student_new

    wide = tokens.astype(jnp.float32)
    normed = (
        wide * lax.rsqrt(jnp.mean(wide * wide, axis=-1, keepdims=True) + 1e-06) * norm_gain
    ).astype(jnp.bfloat16)
    both = jnp.concatenate([normed, lax.ppermute(normed, "core", swap)], axis=0)

    n = n_color // CHUNKS
    for phase in range(2):
        for masks in (FIRST, SECOND):
            got = [exchange(copied[k], DIMS[k][phase], masks) for k in range(COLORS)]
            copied = [jnp.concatenate([a, b], axis=0) for a, b in zip(copied, got)]
    dest = destinations()
    core_at = core.astype(jnp.int32).reshape(1)
    gains = jnp.stack([query_gain, key_gain])
    outputs = ()
    for chunk in range(CHUNKS):
        part = [c[:, :, chunk * n : (chunk + 1) * n] for c in copied]
        one = [exchange(part[k], DIMS[k][2], FIRST) for k in range(COLORS)]
        two = [exchange(part[k], DIMS[k][2], SECOND) for k in range(COLORS)]
        three = [exchange(one[k], DIMS[k][2], SECOND) for k in range(COLORS)]
        units = [u for k in range(COLORS) for u in (part[k], one[k], two[k], three[k])]
        query, key_out, send = project(chunk, dest, core_at, both, gains, units, outputs, n)
        got = lax.ppermute(send, "core", swap)
        outputs = place(chunk, core_at, got, query, key_out, n)
    return (teacher_new, student_new, *outputs)


def solution(mesh):
    split = Mesh(np.asarray(mesh.devices).reshape(2, 2, 4, 4, 2), ("zlo", "core", "y", "x", "zhi"))
    group, fsdp = ("zlo", "core"), ("y", "x", "zhi")
    rows = P(group + fsdp, None)
    return jax.shard_map(
        shards,
        mesh=split,
        in_specs=(rows, P(group, fsdp, None), P(fsdp, group), P(), P(), P()),
        out_specs=(P(fsdp, group), P(fsdp, group), rows, rows),
        check_vma=False,
    )
```

```python
import jax
import jax.numpy as jnp
import numpy as np
from jax import lax
from jax.experimental import pallas as pl
from jax.experimental.pallas import tpu as pltpu
from jax.sharding import Mesh
from jax.sharding import PartitionSpec as P

HEAD = 128
EMA = 0.99
COLORS = 3
PARTS = (384, 128)
FIRST, SECOND = (1, 3), (3, 1)
ORDER = (180, 156)
DIMS = (("x", "y", "z"), ("y", "z", "x"), ("z", "x", "y"))


def exchange(x, dim, masks):
    if dim == "z":
        axes = ("zlo", "core", "zhi")
        pairs = []
        for zlo in range(2):
            for core in range(2):
                for zhi in range(2):
                    z = (2 * zhi + zlo) ^ masks[core]
                    pairs.append(((zlo * 2 + core) * 2 + zhi, ((z % 2) * 2 + core) * 2 + z // 2))
    else:
        axes = ("core", dim)
        pairs = [(core * 4 + i, core * 4 + (i ^ masks[core])) for core in range(2) for i in range(4)]
    return lax.ppermute(x, axes, pairs)


def project_body(colors, n, n_held, *refs):
    _, own, other, gains = refs[:4]
    units = refs[4 : 4 + 4 * len(colors)]
    q_out, k_out, send_out, tok, held, tok_sem, sem = refs[4 + 4 * len(colors) + n_held :]
    half, width = own.shape
    rows = units[0].shape[1]
    order = ORDER[0] + (ORDER[1] - ORDER[0]) * lax.axis_index("core")
    place = {
        "x": lax.axis_index("x"),
        "y": lax.axis_index("y"),
        "z": 2 * lax.axis_index("zhi") + lax.axis_index("zlo"),
    }

    def step(dim, i):
        return lax.bitwise_xor(place[dim], lax.bitwise_and(lax.shift_right_logical(order, 2 * i), 3))

    def fetch(c):
        dims = DIMS[colors[c]]
        for u in range(4):
            src = units[4 * c + u]

            def one(pos, carry):
                at = dict(zip(dims, (step(dims[0], pos % 4), step(dims[1], pos // 4), step(dims[2], jnp.int32(u)))))
                row = (at["y"] * 4 + at["x"]) * 2 + at["z"] // 2
                pltpu.make_async_copy(
                    src.at[pos],
                    held.at[
                        c,
                        pl.ds(pl.multiple_of(row * rows, rows), rows),
                        pl.ds(pl.multiple_of((at["z"] % 2) * n, HEAD), n),
                    ],
                    sem.at[c],
                ).start()
                return carry

            lax.fori_loop(0, 16, one, 0)

    first = pltpu.make_async_copy(own, tok.at[0], tok_sem.at[0])
    second = pltpu.make_async_copy(other, tok.at[1], tok_sem.at[1])
    first.start()
    fetch(0)
    second.start()
    for c in range(1, len(colors)):
        fetch(c)
    scale = width ** (-0.5)
    tile = 256
    for c in range(len(colors)):
        pltpu.make_async_copy(held.at[c], held.at[c], sem.at[c]).wait()
        for t, copy in enumerate((first, second)):
            if c == 0:
                copy.wait()
            for m in range(0, half, tile):
                y = jnp.dot(tok[t, m : m + tile, :], held[c], preferred_element_type=jnp.float32) * scale
                for i, out in enumerate((q_out, k_out)):
                    for h in range(0, n, HEAD):
                        v = y[:, i * n + h : i * n + h + HEAD]
                        v = v * lax.rsqrt(jnp.mean(v * v, axis=-1, keepdims=True) + 1e-06) * gains[i : i + 1, :]
                        v = v.astype(jnp.bfloat16)
                        at = c * n + h
                        if t == 0:
                            out[m : m + tile, at : at + HEAD] = v
                        else:
                            send_out[i, m : m + tile, at : at + HEAD] = v


def project(colors, block, core, own, other, gains, units, outputs):
    half, width = own.shape
    n = units[0].shape[2]
    col = lambda i, core: (0, core[0] * 4 + block)
    wide = n * len(colors)
    any_spec = pl.BlockSpec(memory_space=pl.ANY)
    operands = [own, other, gains, *units]
    specs = [any_spec, any_spec, pl.BlockSpec(gains.shape, lambda *_: (0, 0))] + [any_spec] * len(units)
    aliases = {}
    if outputs:
        aliases = {1 + len(operands): 0, 2 + len(operands): 1}
        operands += list(outputs)
        specs += [any_spec] * 2
    big = jax.ShapeDtypeStruct((half, width), jnp.bfloat16)
    return pl.pallas_call(
        lambda *refs: project_body(colors, n, len(outputs), *refs),
        grid_spec=pltpu.PrefetchScalarGridSpec(
            num_scalar_prefetch=1,
            grid=(1,),
            in_specs=specs,
            out_specs=[
                pl.BlockSpec((half, wide), col),
                pl.BlockSpec((half, wide), col),
                pl.BlockSpec((2, half, wide), lambda *_: (0, 0, 0)),
            ],
            scratch_shapes=[
                pltpu.VMEM((2, half, width), jnp.bfloat16),
                pltpu.VMEM((len(colors), width, 2 * n), jnp.bfloat16),
                pltpu.SemaphoreType.DMA((2,)),
                pltpu.SemaphoreType.DMA((len(colors),)),
            ],
        ),
        out_shape=[big, big, jax.ShapeDtypeStruct((2, half, wide), jnp.bfloat16)],
        input_output_aliases=aliases,
        compiler_params=pltpu.CompilerParams(vmem_limit_bytes=28 * 2**20),
        cost_estimate=pl.CostEstimate(
            flops=2 * 2 * half * width * 2 * wide,
            bytes_accessed=2 * width * (2 * half + 2 * wide),
            transcendentals=0,
        ),
    )(core, *operands)


def place_body(n_got, core, *refs):
    q_out, k_out = refs[n_got + 2 :]
    for i in range(n_got):

        @pl.when(pl.program_id(0) == i)
        def _():
            q_out[...] = refs[i][0]
            k_out[...] = refs[i][1]


def put(block, core, got, query, key_out):
    half = query.shape[0]
    wide = got[0].shape[2]
    col = lambda i, core: (0, (1 - core[0]) * 4 + block + i)
    any_spec = pl.BlockSpec(memory_space=pl.ANY)
    return pl.pallas_call(
        lambda *refs: place_body(len(got), *refs),
        grid_spec=pltpu.PrefetchScalarGridSpec(
            num_scalar_prefetch=1,
            grid=(len(got),),
            in_specs=[pl.BlockSpec(g.shape, lambda *_: (0, 0, 0)) for g in got] + [any_spec, any_spec],
            out_specs=[pl.BlockSpec((half, wide), col), pl.BlockSpec((half, wide), col)],
        ),
        out_shape=[jax.ShapeDtypeStruct(query.shape, query.dtype)] * 2,
        input_output_aliases={1 + len(got): 0, 2 + len(got): 1},
        compiler_params=pltpu.CompilerParams(vmem_limit_bytes=16 * 2**20),
        cost_estimate=pl.CostEstimate(flops=10**9, bytes_accessed=4 * sum(g.size for g in got), transcendentals=0),
    )(core, *got, query, key_out)


def shards(tokens, student, teacher, norm_gain, query_gain, key_gain):
    block = teacher.shape[1]
    core = lax.axis_index("core")
    zlo = lax.axis_index("zlo")
    swap = [(0, 1), (1, 0)]
    part_cols = [[slice(k * PARTS[0], (k + 1) * PARTS[0]), slice(3 * PARTS[0] + k * PARTS[1], 3 * PARTS[0] + (k + 1) * PARTS[1])] for k in range(COLORS)]

    local = student[0]
    blocks = [local[:, j * block : (j + 1) * block] for j in range(4)]
    give = jnp.stack([jnp.where(core == 0, blocks[2 * j + 1], blocks[2 * j]) for j in range(2)])
    got = lax.ppermute(give, "core", swap)
    pair = jnp.stack([jnp.where(core == 0, blocks[2 * j], blocks[2 * j + 1]) for j in range(2)]) + got
    keep = jnp.where(zlo == 0, pair[0], pair[1])
    give = jnp.where(zlo == 0, pair[1], pair[0])
    arrived = []
    for k in range(COLORS):
        cut = jnp.concatenate([give[:, c] for c in part_cols[k]], axis=1)
        arrived.append(lax.ppermute(cut, "zlo", swap))
    owned, copied = [], []
    for k in range(COLORS):
        cut = jnp.concatenate([keep[:, c] for c in part_cols[k]], axis=1)
        if k:
            cut, _ = lax.optimization_barrier((cut, copied[-1]))
        owned.append((cut + arrived[k]) / 4)
        copied.append(owned[-1].astype(jnp.bfloat16)[None])

    wide = tokens.astype(jnp.float32)
    normed = (
        wide * lax.rsqrt(jnp.mean(wide * wide, axis=-1, keepdims=True) + 1e-06) * norm_gain
    ).astype(jnp.bfloat16)
    other = lax.ppermute(normed, "core", swap)

    for phase in range(2):
        for s, masks in enumerate((FIRST, SECOND)):
            got = []
            for k in range(COLORS):
                got.append(exchange(copied[k], DIMS[k][phase], masks))
            if (phase, s) != (1, 1):
                copied = [jnp.concatenate([a, b], axis=0) for a, b in zip(copied, got)]
    units = []
    bounds = ((0, PARTS[0]), (PARTS[0], PARTS[0] + PARTS[1]))
    held = [[jnp.concatenate([a[:, :, lo:hi], b[:, :, lo:hi]], axis=0) for a, b in zip(copied, got)] for lo, hi in bounds]
    for part in range(2):
        one, two, three = [], [], []
        for k in range(COLORS):
            one.append(exchange(held[part][k], DIMS[k][2], FIRST))
            two.append(exchange(held[part][k], DIMS[k][2], SECOND))
            three.append(exchange(one[k], DIMS[k][2], SECOND))
        units.append([[held[part][k], one[k], two[k], three[k]] for k in range(COLORS)])

    core_at = core.astype(jnp.int32).reshape(1)
    gains = jnp.stack([query_gain, key_gain])
    outputs, got = (), []
    for k in range(COLORS):
        *outputs, send = project((k,), k, core_at, normed, other, gains, units[0][k], outputs)
        got.append(lax.ppermute(send, "core", swap))
    *outputs, send = project((0, 1, 2), 3, core_at, normed, other, gains, sum(units[1], []), outputs)
    last = lax.ppermute(send, "core", swap)
    outputs = put(0, core_at, got, *outputs)
    outputs = put(3, core_at, [last], *outputs)

    whole = [owned[k][:, : PARTS[0]] for k in range(COLORS)] + [owned[k][:, PARTS[0] :] for k in range(COLORS)]
    student_new = jnp.concatenate(whole, axis=1)
    teacher_new = EMA * teacher + (1.0 - EMA) * student_new
    return (teacher_new, student_new, *outputs)


def solution(mesh):
    split = Mesh(np.asarray(mesh.devices).reshape(2, 2, 4, 4, 2), ("zlo", "core", "y", "x", "zhi"))
    group, fsdp = ("zlo", "core"), ("y", "x", "zhi")
    rows = P(group + fsdp, None)

    return jax.shard_map(
        shards,
        mesh=split,
        in_specs=(rows, P(group, fsdp, None), P(fsdp, group), P(), P(), P()),
        out_specs=(P(fsdp, group), P(fsdp, group), rows, rows),
        check_vma=False,
    )
```

```python
import jax
import jax.numpy as jnp
import numpy as np
from jax import lax
from jax.experimental import pallas as pl
from jax.experimental.pallas import tpu as pltpu
from jax.sharding import Mesh
from jax.sharding import PartitionSpec as P

HEAD = 128
EMA = 0.99
COLORS = 3
PARTS = 2
VMEM_LIMIT = 16 * 2**20
FIRST, SECOND = (1, 3), (3, 1)
ORDER = (180, 156)
DIMS = (("x", "y", "z"), ("y", "z", "x"), ("z", "x", "y"))


def exchange(x, dim, masks):
    if dim == "z":
        axes = ("zlo", "core", "zhi")
        pairs = []
        for zlo in range(2):
            for core in range(2):
                for zhi in range(2):
                    z = (2 * zhi + zlo) ^ masks[core]
                    pairs.append(((zlo * 2 + core) * 2 + zhi, ((z % 2) * 2 + core) * 2 + z // 2))
    else:
        axes = ("core", dim)
        pairs = [(core * 4 + i, core * 4 + (i ^ masks[core])) for core in range(2) for i in range(4)]
    return lax.ppermute(x, axes, pairs)


def project_body(color, n_held, *refs):
    _, own, other, gains = refs[:4]
    units = refs[4:8]
    q_out, k_out, send_out, held = refs[8 + n_held :]
    half, width = own.shape
    rows, n = units[0].shape[1:]
    order = ORDER[0] + (ORDER[1] - ORDER[0]) * lax.axis_index("core")
    place = {
        "x": lax.axis_index("x"),
        "y": lax.axis_index("y"),
        "z": 2 * lax.axis_index("zhi") + lax.axis_index("zlo"),
    }
    seen = {d: [lax.bitwise_xor(v, lax.bitwise_and(lax.shift_right_logical(order, 2 * i), 3)) for i in range(4)] for d, v in place.items()}
    starts = {
        "x": [(0, v * (2 * rows)) for v in seen["x"]],
        "y": [(0, v * (8 * rows)) for v in seen["y"]],
        "z": [(lax.bitwise_and(v, 1) * n, lax.shift_right_logical(v, 1) * rows) for v in seen["z"]],
    }
    for u in range(4):
        for pos in range(16):
            at = [starts[d][i] for d, i in zip(DIMS[color], (pos % 4, pos // 4, u))]
            col = pl.multiple_of(at[0][0] + at[1][0] + at[2][0], n)
            row = pl.multiple_of(at[0][1] + at[1][1] + at[2][1], rows)
            held[pl.ds(row, rows), pl.ds(col, n)] = units[u][pos]
    scale = width ** (-0.5)
    tile = 256
    for t, src in enumerate((own, other)):
        for m in range(0, half, tile):
            y = jnp.dot(src[m : m + tile, :], held[...], preferred_element_type=jnp.float32) * scale
            for i, out in enumerate((q_out, k_out)):
                for h in range(0, n, HEAD):
                    v = y[:, i * n + h : i * n + h + HEAD]
                    v = v * lax.rsqrt(jnp.mean(v * v, axis=-1, keepdims=True) + 1e-06) * gains[i : i + 1, :]
                    v = v.astype(jnp.bfloat16)
                    if t == 0:
                        out[m : m + tile, h : h + HEAD] = v
                    else:
                        send_out[i, m : m + tile, h : h + HEAD] = v


def project(part, color, where, own, other, gains, units, outputs):
    half, width = own.shape
    n = units[0].shape[2]
    col = lambda i, where: (0, (where[0] * PARTS + part) * COLORS + color)
    any_spec = pl.BlockSpec(memory_space=pl.ANY)
    operands = [own, other, gains, *units, *outputs]
    specs = [pl.BlockSpec(memory_space=pltpu.VMEM)] * (3 + len(units)) + [any_spec] * len(outputs)
    first = 4 + len(units)
    big = jax.ShapeDtypeStruct((half, width), jnp.bfloat16)
    return pl.pallas_call(
        lambda *refs: project_body(color, len(outputs), *refs),
        grid_spec=pltpu.PrefetchScalarGridSpec(
            num_scalar_prefetch=1,
            grid=(1,),
            in_specs=specs,
            out_specs=[
                pl.BlockSpec((half, n), col),
                pl.BlockSpec((half, n), col),
                pl.BlockSpec((2, half, n), lambda *_: (0, 0, 0)),
            ],
            scratch_shapes=[pltpu.VMEM((width, 2 * n), jnp.bfloat16)],
        ),
        out_shape=[big, big, jax.ShapeDtypeStruct((2, half, n), jnp.bfloat16)],
        input_output_aliases={first: 0, first + 1: 1} if outputs else {},
        compiler_params=pltpu.CompilerParams(vmem_limit_bytes=VMEM_LIMIT),
        cost_estimate=pl.CostEstimate(
            flops=2 * 2 * half * width * 2 * n,
            bytes_accessed=2 * width * (2 * half + 2 * n),
            transcendentals=0,
        ),
    )(where, *operands)


def put_body(where, *refs):
    q_out, k_out = refs[COLORS + 2 :]
    n = refs[0].shape[2]
    for k in range(COLORS):
        q_out[:, k * n : (k + 1) * n] = refs[k][0]
        k_out[:, k * n : (k + 1) * n] = refs[k][1]


def put(part, where, got, query, key_out):
    _, half, n = got[0].shape
    rows = half // 4
    col = lambda i, where: (i, (1 - where[0]) * PARTS + part)
    any_spec = pl.BlockSpec(memory_space=pl.ANY)
    return pl.pallas_call(
        put_body,
        grid_spec=pltpu.PrefetchScalarGridSpec(
            num_scalar_prefetch=1,
            grid=(half // rows,),
            in_specs=[pl.BlockSpec((2, rows, n), lambda i, *_: (0, i, 0))] * COLORS + [any_spec, any_spec],
            out_specs=[pl.BlockSpec((rows, COLORS * n), col)] * 2,
        ),
        out_shape=[jax.ShapeDtypeStruct(query.shape, query.dtype)] * 2,
        input_output_aliases={COLORS + 1: 0, COLORS + 2: 1},
        compiler_params=pltpu.CompilerParams(vmem_limit_bytes=8 * 2**20),
        cost_estimate=pl.CostEstimate(flops=10**9, bytes_accessed=8 * COLORS * got[0].size, transcendentals=0),
    )(where, *got, query, key_out)


def join_body(n, a, b, *outs):
    for p, out in enumerate(outs):
        out[0] = a[:, :, p * n : (p + 1) * n]
        out[1] = b[:, :, p * n : (p + 1) * n]


def join(a, b):
    places, rows, width = a.shape
    n = width // PARTS
    step = 2
    made = pl.pallas_call(
        lambda *refs: join_body(n, *refs),
        grid=(places // step,),
        in_specs=[pl.BlockSpec((step, rows, width), lambda i: (i, 0, 0))] * 2,
        out_specs=[pl.BlockSpec((2, step, rows, n), lambda i: (0, i, 0, 0))] * PARTS,
        out_shape=[jax.ShapeDtypeStruct((2, places, rows, n), a.dtype)] * PARTS,
        compiler_params=pltpu.CompilerParams(vmem_limit_bytes=8 * 2**20),
        cost_estimate=pl.CostEstimate(flops=10**9, bytes_accessed=8 * a.size, transcendentals=0),
        name="join",
    )(a, b)
    return [m.reshape(2 * places, rows, n) for m in made]


def pick_body(core, local, out):
    out[0] = local[...]


def pick(core, local, block):
    rows = local.shape[0]
    return pl.pallas_call(
        pick_body,
        grid_spec=pltpu.PrefetchScalarGridSpec(
            num_scalar_prefetch=1,
            grid=(2,),
            in_specs=[pl.BlockSpec((rows, block), lambda j, core: (0, 2 * j + 1 - core[0]))],
            out_specs=pl.BlockSpec((1, rows, block), lambda j, core: (j, 0, 0)),
        ),
        out_shape=jax.ShapeDtypeStruct((2, rows, block), jnp.float32),
        compiler_params=pltpu.CompilerParams(vmem_limit_bytes=8 * 2**20),
        cost_estimate=pl.CostEstimate(flops=10**9, bytes_accessed=16 * rows * block, transcendentals=0),
        name="pick",
    )(core, local)


def merge_body(n, where, local, got, keep, *give):
    total = local[...] + got[0]
    mine = pl.program_id(0) == where[1]

    @pl.when(mine)
    def _():
        keep[...] = total

    @pl.when(jnp.logical_not(mine))
    def _():
        for k in range(COLORS):
            for p in range(PARTS):
                at = (p * COLORS + k) * n // PARTS
                give[k][:, p * n // PARTS : (p + 1) * n // PARTS] = total[:, at : at + n // PARTS]


def merge(where, local, got):
    _, rows, block = got.shape
    n = block // COLORS
    return pl.pallas_call(
        lambda *refs: merge_body(n, *refs),
        grid_spec=pltpu.PrefetchScalarGridSpec(
            num_scalar_prefetch=1,
            grid=(2,),
            in_specs=[
                pl.BlockSpec((rows, block), lambda j, where: (0, 2 * j + where[0])),
                pl.BlockSpec((1, rows, block), lambda j, where: (j, 0, 0)),
            ],
            out_specs=[pl.BlockSpec((rows, block), lambda *_: (0, 0))] + [pl.BlockSpec((rows, n), lambda *_: (0, 0))] * COLORS,
        ),
        out_shape=[jax.ShapeDtypeStruct((rows, block), jnp.float32)] + [jax.ShapeDtypeStruct((rows, n), jnp.float32)] * COLORS,
        compiler_params=pltpu.CompilerParams(vmem_limit_bytes=16 * 2**20),
        cost_estimate=pl.CostEstimate(flops=10**9, bytes_accessed=24 * rows * block, transcendentals=0),
        name="merge",
    )(where, local, got)


def shards(tokens, student, teacher, norm_gain, query_gain, key_gain):
    block = teacher.shape[1]
    n = block // COLORS
    core = lax.axis_index("core")
    where = jnp.stack([core, lax.axis_index("zlo")]).astype(jnp.int32)
    swap = [(0, 1), (1, 0)]

    local = student[0]
    got = lax.ppermute(pick(where, local, block), "core", swap)
    keep, *give = merge(where, local, got)
    arrived, owned, copied = [], [], []
    for k in range(COLORS):
        arrived.append(lax.ppermute(give[k], "zlo", swap))
    for k in range(COLORS):
        spans = [(p * COLORS + k) * n // PARTS for p in range(PARTS)]
        cut = jnp.concatenate([keep[:, at : at + n // PARTS] for at in spans], axis=1)
        if k:
            cut, _ = lax.optimization_barrier((cut, copied[-1]))
        owned.append((cut + arrived[k]) / 4)
        copied.append(owned[k].astype(jnp.bfloat16)[None])
    student_new = jnp.concatenate(
        [o[:, p * n // PARTS : (p + 1) * n // PARTS] for p in range(PARTS) for o in owned], axis=1
    )
    teacher_new = EMA * teacher + (1.0 - EMA) * student_new

    wide = tokens.astype(jnp.float32)
    normed = (
        wide * lax.rsqrt(jnp.mean(wide * wide, axis=-1, keepdims=True) + 1e-06) * norm_gain
    ).astype(jnp.bfloat16)
    other = lax.ppermute(normed, "core", swap)

    parts = [None] * COLORS
    for s in range(4):
        for k in range(COLORS):
            got = exchange(copied[k], DIMS[k][s // 2], (FIRST, SECOND)[s % 2])
            if s < 3:
                copied[k] = jnp.concatenate([copied[k], got], axis=0)
            else:
                parts[k] = join(copied[k], got)
    gains = jnp.stack([query_gain, key_gain])
    where, student_new, teacher_new = lax.optimization_barrier((where, student_new, teacher_new))
    outputs, back = (), []
    for p in range(PARTS):
        back.append([])
        for k in range(COLORS):
            one = exchange(parts[k][p], DIMS[k][2], FIRST)
            two = exchange(parts[k][p], DIMS[k][2], SECOND)
            three = exchange(one, DIMS[k][2], SECOND)
            units = [parts[k][p], one, two, three]
            *outputs, send = project(p, k, where, normed, other, gains, units, outputs)
            back[p].append(lax.ppermute(send, "core", swap))
    for p in range(PARTS):
        outputs = put(p, where, back[p], *outputs)
    return (teacher_new, student_new, *outputs)


def solution(mesh):
    split = Mesh(np.asarray(mesh.devices).reshape(2, 2, 4, 4, 2), ("zlo", "core", "y", "x", "zhi"))
    group, fsdp = ("zlo", "core"), ("y", "x", "zhi")
    rows = P(group + fsdp, None)

    return jax.shard_map(
        shards,
        mesh=split,
        in_specs=(rows, P(group, fsdp, None), P(fsdp, group), P(), P(), P()),
        out_specs=(P(fsdp, group), P(fsdp, group), rows, rows),
        check_vma=False,
    )
```

```python
import jax
import jax.numpy as jnp
import numpy as np
from jax import lax
from jax.experimental import pallas as pl
from jax.experimental.pallas import tpu as pltpu
from jax.sharding import Mesh
from jax.sharding import PartitionSpec as P

HEAD = 128
EMA = 0.99
COLORS = 3
VMEM_LIMIT = 20 * 2**20
TILE = 256
FIRST, SECOND = (1, 3), (3, 1)
ORDER = (180, 156)
DIMS = (("x", "y", "z"), ("y", "z", "x"), ("z", "x", "y"))


def exchange(x, dim, masks):
    if dim == "z":
        axes = ("zlo", "core", "zhi")
        pairs = []
        for zlo in range(2):
            for core in range(2):
                for zhi in range(2):
                    z = (2 * zhi + zlo) ^ masks[core]
                    pairs.append(((zlo * 2 + core) * 2 + zhi, ((z % 2) * 2 + core) * 2 + z // 2))
    else:
        axes = ("core", dim)
        pairs = [(core * 4 + i, core * 4 + (i ^ masks[core])) for core in range(2) for i in range(4)]
    return lax.ppermute(x, axes, pairs)


def fill(color, half, units, held, n):
    core = lax.axis_index("core")
    order = ORDER[0] + (ORDER[1] - ORDER[0]) * core
    dims = DIMS[color]
    place = {
        "x": lax.axis_index("x"),
        "y": lax.axis_index("y"),
        "z": 2 * lax.axis_index("zhi") + lax.axis_index("zlo"),
    }
    seen = {d: [lax.bitwise_xor(v, lax.bitwise_and(lax.shift_right_logical(order, 2 * i), 3)) for i in range(4)] for d, v in place.items()}
    low = lambda v: lax.bitwise_and(v, 1)
    high = lambda v: lax.shift_right_logical(v, 1)
    rows = units[0].shape[1]
    if dims[2] == "z":
        row_of = {"x": lambda v: v * 2, "y": lambda v: v * 8, "z": high}
    elif dims[2] == "x":
        row_of = {"x": lambda v: low(v) * 2, "y": lambda v: v * 4, "z": high}
    else:
        row_of = {"x": lambda v: v * 2, "y": lambda v: low(v) * 8, "z": high}
    at_row = {d: [row_of[d](v) * rows for v in seen[d]] for d in dims}
    at_col = [0 if dims[2] == "z" else low(v) * n for v in seen["z"]]

    def copy(u):
        for pos in range(16):
            i = dict(zip(dims, (pos % 4, pos // 4, u)))
            row = pl.multiple_of(at_row["x"][i["x"]] + at_row["y"][i["y"]] + at_row["z"][i["z"]], rows)
            col = at_col[i["z"]]
            col = col if isinstance(col, int) else pl.multiple_of(col, n)
            held[pl.ds(row, rows), pl.ds(col, n)] = units[u][pos]

    if dims[2] == "z":
        for u in ((1, 2), (0, 3))[half]:
            copy(u)
    else:
        copy((0, 3)[half])
        for u in (1, 2):
            pl.when(core == (u - 1 if half == 0 else 2 - u))(lambda u=u: copy(u))


def tokens_of(color, half, src, m):
    last = DIMS[color][2]
    span = slice(m, m + TILE)
    if last == "z":
        return src[span, :]
    width = src.shape[1]
    side = lax.bitwise_xor(lax.shift_right_logical(lax.axis_index(last), 1), half)
    if last == "y":
        return src[span, pl.ds(pl.multiple_of(side * (width // 2), HEAD), width // 2)]
    cut = width // 8
    return jnp.concatenate(
        [src[span, pl.ds(pl.multiple_of(side * cut + y * 2 * cut, HEAD), cut)] for y in range(4)], axis=1
    )


def head_norm(v, gain):
    v = v * lax.rsqrt(jnp.mean(v * v, axis=-1, keepdims=True) + 1e-06) * gain
    return v.astype(jnp.bfloat16)


def begin_body(color, where, own, other, gains, *refs):
    units, (out, held) = refs[:4], refs[4:]
    n = units[0].shape[2]
    fill(color, 0, units, held, n)
    for t, src in enumerate((own, other)):
        for m in range(0, own.shape[0], TILE):
            y = jnp.dot(tokens_of(color, 0, src, m), held[...], preferred_element_type=jnp.float32)
            if DIMS[color][2] == "z":
                y = y * own.shape[1] ** (-0.5)
                gain = jnp.where(where[1] == 0, gains[1:2, :], gains[0:1, :])
                for h in range(0, n, HEAD):
                    out[t, m : m + TILE, h : h + HEAD] = head_norm(y[:, h : h + HEAD], gain)
            else:
                out[t, m : m + TILE, :] = y


def end_body(color, n_held, where, own, other, gains, begun, *refs):
    units = refs[:4]
    q_out, k_out, send_out, held = refs[4 + n_held :]
    n = units[0].shape[2]
    scale = own.shape[1] ** (-0.5)
    fill(color, 1, units, held, n)
    for t, src in enumerate((own, other)):
        for m in range(0, own.shape[0], TILE):
            span = slice(m, m + TILE)
            y = jnp.dot(tokens_of(color, 1, src, m), held[...], preferred_element_type=jnp.float32)
            outs = (q_out, k_out) if t == 0 else (send_out.at[0], send_out.at[1])
            if DIMS[color][2] == "z":
                y = y * scale
                gain = jnp.where(where[1] == 0, gains[0:1, :], gains[1:2, :])
                mine = jnp.concatenate([head_norm(y[:, h : h + HEAD], gain) for h in range(0, n, HEAD)], axis=1)
                early = begun[t, span, :]
                for i, out in enumerate(outs):

                    @pl.when(where[1] == i)
                    def _():
                        out[span, :] = mine

                    @pl.when(where[1] != i)
                    def _():
                        out[span, :] = early
            else:
                y = (y + begun[t, span, :]) * scale
                for i, out in enumerate(outs):
                    for h in range(0, n, HEAD):
                        out[span, h : h + HEAD] = head_norm(y[:, i * n + h : i * n + h + HEAD], gains[i : i + 1, :])


def project_half(color, half, where, own, other, gains, units, begun=None, outputs=()):
    tokens, width = own.shape
    n = units[0].shape[2]
    vmem, any_spec = pl.BlockSpec(memory_space=pltpu.VMEM), pl.BlockSpec(memory_space=pl.ANY)
    operands = [own, other, gains, *([] if half == 0 else [begun]), *units, *outputs]
    specs = [vmem] * (len(operands) - len(outputs)) + [any_spec] * len(outputs)
    by_block = DIMS[color][2] == "z"
    whole = lambda *shape: pl.BlockSpec(shape, lambda i, *_: (0,) * len(shape))
    if half == 0:
        body = lambda *refs: begin_body(color, *refs)
        out_shape = [jax.ShapeDtypeStruct((2, tokens, n), jnp.bfloat16) if by_block else jax.ShapeDtypeStruct((2, tokens, 2 * n), jnp.float32)]
        out_specs = [vmem]
        aliases = {}
    else:
        body = lambda *refs: end_body(color, len(outputs), *refs)
        big = jax.ShapeDtypeStruct((tokens, width), jnp.bfloat16)
        out_shape = [big, big, jax.ShapeDtypeStruct((2, tokens, n), jnp.bfloat16)]
        col = lambda i, where: (0, where[0] * COLORS + color)
        out_specs = [pl.BlockSpec((tokens, n), col), pl.BlockSpec((tokens, n), col), whole(2, tokens, n)]
        first = 1 + len(operands) - len(outputs)
        aliases = {first: 0, first + 1: 1} if outputs else {}
    return pl.pallas_call(
        body,
        grid_spec=pltpu.PrefetchScalarGridSpec(
            num_scalar_prefetch=1,
            grid=(1,),
            in_specs=specs,
            out_specs=out_specs,
            scratch_shapes=[pltpu.VMEM((width, n) if by_block else (width // 2, 2 * n), jnp.bfloat16)],
        ),
        out_shape=out_shape,
        input_output_aliases=aliases,
        compiler_params=pltpu.CompilerParams(vmem_limit_bytes=VMEM_LIMIT),
        cost_estimate=pl.CostEstimate(
            flops=2 * 2 * tokens * width * n,
            bytes_accessed=2 * width * (2 * tokens + 2 * n),
            transcendentals=0,
        ),
    )(where, *operands)


def put_body(where, got, q_in, k_in, q_out, k_out):
    q_out[...] = got[0]
    k_out[...] = got[1]


def put(color, where, got, query, key_out):
    _, half, n = got.shape
    col = lambda i, where: (i, (1 - where[0]) * COLORS + color)
    any_spec = pl.BlockSpec(memory_space=pl.ANY)
    return pl.pallas_call(
        put_body,
        grid_spec=pltpu.PrefetchScalarGridSpec(
            num_scalar_prefetch=1,
            grid=(2,),
            in_specs=[pl.BlockSpec((2, half // 2, n), lambda i, *_: (0, i, 0)), any_spec, any_spec],
            out_specs=[pl.BlockSpec((half // 2, n), col)] * 2,
        ),
        out_shape=[jax.ShapeDtypeStruct(query.shape, query.dtype)] * 2,
        input_output_aliases={2: 0, 3: 1},
        compiler_params=pltpu.CompilerParams(vmem_limit_bytes=8 * 2**20),
        cost_estimate=pl.CostEstimate(flops=10**9, bytes_accessed=8 * got.size, transcendentals=0),
    )(where, got, query, key_out)


def pick_body(core, local, out):
    out[0] = local[...]


def pick(core, local, block):
    rows = local.shape[0]
    return pl.pallas_call(
        pick_body,
        grid_spec=pltpu.PrefetchScalarGridSpec(
            num_scalar_prefetch=1,
            grid=(2,),
            in_specs=[pl.BlockSpec((rows, block), lambda j, core: (0, 2 * j + 1 - core[0]))],
            out_specs=pl.BlockSpec((1, rows, block), lambda j, core: (j, 0, 0)),
        ),
        out_shape=jax.ShapeDtypeStruct((2, rows, block), jnp.float32),
        compiler_params=pltpu.CompilerParams(vmem_limit_bytes=8 * 2**20),
        cost_estimate=pl.CostEstimate(flops=10**9, bytes_accessed=16 * rows * block, transcendentals=0),
        name="pick",
    )(core, local)


def merge_body(n, where, local, got, keep, rest, *give):
    total = local[...] + got[0]
    mine = pl.program_id(0) == where[1]

    @pl.when(mine)
    def _():
        keep[...] = total

    @pl.when(jnp.logical_not(mine))
    def _():
        high = total.astype(jnp.bfloat16)
        rest[...] = (total - high.astype(jnp.float32)).astype(jnp.bfloat16)
        for k in range(COLORS):
            give[k][...] = high[:, k * n : (k + 1) * n]


def merge(where, local, got):
    _, rows, block = got.shape
    n = block // COLORS
    return pl.pallas_call(
        lambda *refs: merge_body(n, *refs),
        grid_spec=pltpu.PrefetchScalarGridSpec(
            num_scalar_prefetch=1,
            grid=(2,),
            in_specs=[
                pl.BlockSpec((rows, block), lambda j, where: (0, 2 * j + where[0])),
                pl.BlockSpec((1, rows, block), lambda j, where: (j, 0, 0)),
            ],
            out_specs=[pl.BlockSpec((rows, block), lambda *_: (0, 0))] * 2 + [pl.BlockSpec((rows, n), lambda *_: (0, 0))] * COLORS,
        ),
        out_shape=[jax.ShapeDtypeStruct((rows, block), jnp.float32), jax.ShapeDtypeStruct((rows, block), jnp.bfloat16)]
        + [jax.ShapeDtypeStruct((rows, n), jnp.bfloat16)] * COLORS,
        compiler_params=pltpu.CompilerParams(vmem_limit_bytes=16 * 2**20),
        cost_estimate=pl.CostEstimate(flops=10**9, bytes_accessed=24 * rows * block, transcendentals=0),
        name="merge",
    )(where, local, got)


def shards(tokens, student, teacher, norm_gain, query_gain, key_gain):
    block = teacher.shape[1]
    n = block // COLORS
    core = lax.axis_index("core")
    where = jnp.stack([core, lax.axis_index("zlo")]).astype(jnp.int32)
    swap = [(0, 1), (1, 0)]

    local = student[0]
    got = lax.ppermute(pick(where, local, block), "core", swap)
    keep, rest, *give = merge(where, local, got)
    arrived, copied = [], []
    for k in range(COLORS):
        arrived.append(lax.ppermute(give[k], "zlo", swap).astype(jnp.float32))
    rest = lax.ppermute(rest, "zlo", swap).astype(jnp.float32)
    for k in range(COLORS):
        cut = keep[:, k * n : (k + 1) * n]
        if k:
            cut, _ = lax.optimization_barrier((cut, copied[-1]))
        copied.append(((cut + arrived[k]) / 4).astype(jnp.bfloat16)[None])
    high = jnp.concatenate(arrived, axis=1)
    student_new = (keep + (high + rest)) / 4
    teacher_new = EMA * teacher + (1.0 - EMA) * student_new

    wide = tokens.astype(jnp.float32)
    normed = (
        wide * lax.rsqrt(jnp.mean(wide * wide, axis=-1, keepdims=True) + 1e-06) * norm_gain
    ).astype(jnp.bfloat16)
    other = lax.ppermute(normed, "core", swap)

    for s in range(4):
        for k in range(COLORS):
            got = exchange(copied[k], DIMS[k][s // 2], (FIRST, SECOND)[s % 2])
            copied[k] = jnp.concatenate([copied[k], got], axis=0)
    gains = jnp.stack([query_gain, key_gain])
    units, begun = [], []
    for k in range(COLORS):
        one = exchange(copied[k], DIMS[k][2], FIRST)
        two = exchange(copied[k], DIMS[k][2], SECOND)
        three = exchange(one, DIMS[k][2], SECOND)
        units.append([copied[k], one, two, three])
        begun += project_half(k, 0, where, normed, other, gains, [copied[k], one, two, copied[k]])
    outputs, back = (), []
    for k in range(COLORS):
        *outputs, send = project_half(k, 1, where, normed, other, gains, units[k], begun[k], outputs)
        back.append(lax.ppermute(send, "core", swap))
    where, student_new, teacher_new = lax.optimization_barrier((where, student_new, teacher_new))
    for k in range(COLORS):
        outputs = put(k, where, back[k], *outputs)
    return (teacher_new, student_new, *outputs)


def solution(mesh):
    split = Mesh(np.asarray(mesh.devices).reshape(2, 2, 4, 4, 2), ("zlo", "core", "y", "x", "zhi"))
    group, fsdp = ("zlo", "core"), ("y", "x", "zhi")
    rows = P(group + fsdp, None)

    return jax.shard_map(
        shards,
        mesh=split,
        in_specs=(rows, P(group, fsdp, None), P(fsdp, group), P(), P(), P()),
        out_specs=(P(fsdp, group), P(fsdp, group), rows, rows),
        check_vma=False,
    )
```

```python
import jax
import jax.numpy as jnp
import numpy as np
from jax import lax
from jax.experimental import pallas as pl
from jax.experimental.pallas import tpu as pltpu
from jax.sharding import Mesh
from jax.sharding import PartitionSpec as P

HEAD = 128
EMA = 0.99
COLORS = 3
VMEM_LIMIT = 20 * 2**20
TILE = 256
FIRST, SECOND = (1, 3), (3, 1)
ORDER = (180, 156)
DIMS = (("x", "y", "z"), ("y", "z", "x"), ("z", "x", "y"))


def exchange(x, dim, masks):
    if dim == "z":
        axes = ("zlo", "core", "zhi")
        pairs = []
        for zlo in range(2):
            for core in range(2):
                for zhi in range(2):
                    z = (2 * zhi + zlo) ^ masks[core]
                    pairs.append(((zlo * 2 + core) * 2 + zhi, ((z % 2) * 2 + core) * 2 + z // 2))
    else:
        axes = ("core", dim)
        pairs = [(core * 4 + i, core * 4 + (i ^ masks[core])) for core in range(2) for i in range(4)]
    return lax.ppermute(x, axes, pairs)


def fill(color, half, units, held, n):
    core = lax.axis_index("core")
    order = ORDER[0] + (ORDER[1] - ORDER[0]) * core
    dims = DIMS[color]
    place = {
        "x": lax.axis_index("x"),
        "y": lax.axis_index("y"),
        "z": 2 * lax.axis_index("zhi") + lax.axis_index("zlo"),
    }
    seen = {d: [lax.bitwise_xor(v, lax.bitwise_and(lax.shift_right_logical(order, 2 * i), 3)) for i in range(4)] for d, v in place.items()}
    low = lambda v: lax.bitwise_and(v, 1)
    high = lambda v: lax.shift_right_logical(v, 1)
    rows = units[0].shape[1]
    if dims[2] == "z":
        row_of = {"x": lambda v: v * 2, "y": lambda v: v * 8, "z": high}
    elif dims[2] == "x":
        row_of = {"x": lambda v: low(v) * 2, "y": lambda v: v * 4, "z": high}
    else:
        row_of = {"x": lambda v: v * 2, "y": lambda v: low(v) * 8, "z": high}
    at_row = {d: [row_of[d](v) * rows for v in seen[d]] for d in dims}
    at_col = [0 if dims[2] == "z" else low(v) * n for v in seen["z"]]

    def copy(u):
        for pos in range(16):
            i = dict(zip(dims, (pos % 4, pos // 4, u)))
            row = pl.multiple_of(at_row["x"][i["x"]] + at_row["y"][i["y"]] + at_row["z"][i["z"]], rows)
            col = at_col[i["z"]]
            col = col if isinstance(col, int) else pl.multiple_of(col, n)
            held[pl.ds(row, rows), pl.ds(col, n)] = units[u][pos]

    if dims[2] == "z":
        for u in ((1, 2), (0, 3))[half]:
            copy(u)
    else:
        copy((0, 3)[half])
        for u in (1, 2):
            pl.when(core == (u - 1 if half == 0 else 2 - u))(lambda u=u: copy(u))


def tokens_of(color, half, src, m):
    last = DIMS[color][2]
    span = slice(m, m + TILE)
    if last == "z":
        return src[span, :]
    width = src.shape[1]
    side = lax.bitwise_xor(lax.shift_right_logical(lax.axis_index(last), 1), half)
    if last == "y":
        return src[span, pl.ds(pl.multiple_of(side * (width // 2), HEAD), width // 2)]
    cut = width // 8
    return jnp.concatenate(
        [src[span, pl.ds(pl.multiple_of(side * cut + y * 2 * cut, HEAD), cut)] for y in range(4)], axis=1
    )


def head_norm(v, gain):
    v = v * lax.rsqrt(jnp.mean(v * v, axis=-1, keepdims=True) + 1e-06) * gain
    return v.astype(jnp.bfloat16)


def begin_body(color, where, own, other, gains, *refs):
    units, (out, held) = refs[:4], refs[4:]
    n = units[0].shape[2]
    fill(color, 0, units, held, n)
    for t, src in enumerate((own, other)):
        for m in range(0, own.shape[0], TILE):
            y = jnp.dot(tokens_of(color, 0, src, m), held[...], preferred_element_type=jnp.float32)
            if DIMS[color][2] == "z":
                y = y * own.shape[1] ** (-0.5)
                gain = jnp.where(where[1] == 0, gains[1:2, :], gains[0:1, :])
                for h in range(0, n, HEAD):
                    out[t, m : m + TILE, h : h + HEAD] = head_norm(y[:, h : h + HEAD], gain)
            else:
                out[t, m : m + TILE, :] = y


def end_body(color, n_held, where, own, other, gains, begun, *refs):
    units = refs[:4]
    q_out, k_out, send_out, held = refs[4 + n_held :]
    n = units[0].shape[2]
    scale = own.shape[1] ** (-0.5)
    fill(color, 1, units, held, n)
    for t, src in enumerate((own, other)):
        for m in range(0, own.shape[0], TILE):
            span = slice(m, m + TILE)
            y = jnp.dot(tokens_of(color, 1, src, m), held[...], preferred_element_type=jnp.float32)
            outs = (q_out, k_out) if t == 0 else (send_out.at[0], send_out.at[1])
            if DIMS[color][2] == "z":
                y = y * scale
                gain = jnp.where(where[1] == 0, gains[0:1, :], gains[1:2, :])
                mine = jnp.concatenate([head_norm(y[:, h : h + HEAD], gain) for h in range(0, n, HEAD)], axis=1)
                early = begun[t, span, :]
                for i, out in enumerate(outs):
                    out[span, :] = jnp.where(where[1] == i, mine, early)
            else:
                y = (y + begun[t, span, :]) * scale
                for i, out in enumerate(outs):
                    for h in range(0, n, HEAD):
                        out[span, h : h + HEAD] = head_norm(y[:, i * n + h : i * n + h + HEAD], gains[i : i + 1, :])


def project_half(color, half, where, own, other, gains, units, begun=None, outputs=()):
    tokens, width = own.shape
    n = units[0].shape[2]
    vmem, any_spec = pl.BlockSpec(memory_space=pltpu.VMEM), pl.BlockSpec(memory_space=pl.ANY)
    operands = [own, other, gains, *([] if half == 0 else [begun]), *units, *outputs]
    specs = [vmem] * (len(operands) - len(outputs)) + [any_spec] * len(outputs)
    by_block = DIMS[color][2] == "z"
    whole = lambda *shape: pl.BlockSpec(shape, lambda i, *_: (0,) * len(shape))
    if half == 0:
        body = lambda *refs: begin_body(color, *refs)
        out_shape = [jax.ShapeDtypeStruct((2, tokens, n), jnp.bfloat16) if by_block else jax.ShapeDtypeStruct((2, tokens, 2 * n), jnp.float32)]
        out_specs = [vmem]
        aliases = {}
    else:
        body = lambda *refs: end_body(color, len(outputs), *refs)
        big = jax.ShapeDtypeStruct((tokens, width), jnp.bfloat16)
        out_shape = [big, big, jax.ShapeDtypeStruct((2, tokens, n), jnp.bfloat16)]
        col = lambda i, where: (0, where[0] * COLORS + color)
        out_specs = [pl.BlockSpec((tokens, n), col), pl.BlockSpec((tokens, n), col), whole(2, tokens, n)]
        first = 1 + len(operands) - len(outputs)
        aliases = {first: 0, first + 1: 1} if outputs else {}
    return pl.pallas_call(
        body,
        grid_spec=pltpu.PrefetchScalarGridSpec(
            num_scalar_prefetch=1,
            grid=(1,),
            in_specs=specs,
            out_specs=out_specs,
            scratch_shapes=[pltpu.VMEM((width, n) if by_block else (width // 2, 2 * n), jnp.bfloat16)],
        ),
        out_shape=out_shape,
        input_output_aliases=aliases,
        compiler_params=pltpu.CompilerParams(vmem_limit_bytes=VMEM_LIMIT),
        cost_estimate=pl.CostEstimate(
            flops=2 * 2 * tokens * width * n,
            bytes_accessed=2 * width * (2 * tokens + 2 * n),
            transcendentals=0,
        ),
    )(where, *operands)


def put_body(n_got, where, *refs):
    q_out, k_out = refs[n_got + 2 :]
    for i in range(n_got):

        @pl.when(pl.program_id(0) == i)
        def _():
            q_out[...] = refs[i][0]
            k_out[...] = refs[i][1]


def put(color, where, got, query, key_out):
    _, half, n = got[0].shape
    col = lambda i, where: (0, (1 - where[0]) * COLORS + color + i)
    any_spec = pl.BlockSpec(memory_space=pl.ANY)
    return pl.pallas_call(
        lambda *refs: put_body(len(got), *refs),
        grid_spec=pltpu.PrefetchScalarGridSpec(
            num_scalar_prefetch=1,
            grid=(len(got),),
            in_specs=[pl.BlockSpec((2, half, n), lambda *_: (0, 0, 0))] * len(got) + [any_spec, any_spec],
            out_specs=[pl.BlockSpec((half, n), col)] * 2,
        ),
        out_shape=[jax.ShapeDtypeStruct(query.shape, query.dtype)] * 2,
        input_output_aliases={1 + len(got): 0, 2 + len(got): 1},
        compiler_params=pltpu.CompilerParams(vmem_limit_bytes=12 * 2**20),
        cost_estimate=pl.CostEstimate(flops=10**9, bytes_accessed=8 * len(got) * got[0].size, transcendentals=0),
    )(where, *got, query, key_out)


def pick_body(core, local, out):
    out[0] = local[...]


def pick(core, local, block):
    rows = local.shape[0]
    return pl.pallas_call(
        pick_body,
        grid_spec=pltpu.PrefetchScalarGridSpec(
            num_scalar_prefetch=1,
            grid=(2,),
            in_specs=[pl.BlockSpec((rows, block), lambda j, core: (0, 2 * j + 1 - core[0]))],
            out_specs=pl.BlockSpec((1, rows, block), lambda j, core: (j, 0, 0)),
        ),
        out_shape=jax.ShapeDtypeStruct((2, rows, block), jnp.float32),
        compiler_params=pltpu.CompilerParams(vmem_limit_bytes=8 * 2**20),
        cost_estimate=pl.CostEstimate(flops=10**9, bytes_accessed=16 * rows * block, transcendentals=0),
        name="pick",
    )(core, local)


def merge_body(n, where, local, got, keep, rest, *give):
    total = local[...] + got[0]
    mine = pl.program_id(0) == where[1]

    @pl.when(mine)
    def _():
        keep[...] = total

    @pl.when(jnp.logical_not(mine))
    def _():
        high = total.astype(jnp.bfloat16)
        rest[...] = (total - high.astype(jnp.float32)).astype(jnp.bfloat16)
        for k in range(COLORS):
            give[k][...] = high[:, k * n : (k + 1) * n]


def merge(where, local, got):
    _, rows, block = got.shape
    n = block // COLORS
    return pl.pallas_call(
        lambda *refs: merge_body(n, *refs),
        grid_spec=pltpu.PrefetchScalarGridSpec(
            num_scalar_prefetch=1,
            grid=(2,),
            in_specs=[
                pl.BlockSpec((rows, block), lambda j, where: (0, 2 * j + where[0])),
                pl.BlockSpec((1, rows, block), lambda j, where: (j, 0, 0)),
            ],
            out_specs=[pl.BlockSpec((rows, block), lambda *_: (0, 0))] * 2 + [pl.BlockSpec((rows, n), lambda *_: (0, 0))] * COLORS,
        ),
        out_shape=[jax.ShapeDtypeStruct((rows, block), jnp.float32), jax.ShapeDtypeStruct((rows, block), jnp.bfloat16)]
        + [jax.ShapeDtypeStruct((rows, n), jnp.bfloat16)] * COLORS,
        compiler_params=pltpu.CompilerParams(vmem_limit_bytes=16 * 2**20),
        cost_estimate=pl.CostEstimate(flops=10**9, bytes_accessed=24 * rows * block, transcendentals=0),
        name="merge",
    )(where, local, got)


def shards(tokens, student, teacher, norm_gain, query_gain, key_gain):
    block = teacher.shape[1]
    n = block // COLORS
    core = lax.axis_index("core")
    where = jnp.stack([core, lax.axis_index("zlo")]).astype(jnp.int32)
    swap = [(0, 1), (1, 0)]

    local = student[0]
    got = lax.ppermute(pick(where, local, block), "core", swap)
    keep, rest, *give = merge(where, local, got)
    arrived, copied = [], []
    for k in range(COLORS):
        arrived.append(lax.ppermute(give[k], "zlo", swap).astype(jnp.float32))
    rest = lax.ppermute(rest, "zlo", swap).astype(jnp.float32)
    for k in range(COLORS):
        cut = keep[:, k * n : (k + 1) * n]
        if k:
            cut, _ = lax.optimization_barrier((cut, copied[-1]))
        copied.append(((cut + arrived[k]) / 4).astype(jnp.bfloat16)[None])
    high = jnp.concatenate(arrived, axis=1)
    student_new = (keep + (high + rest)) / 4
    teacher_new = EMA * teacher + (1.0 - EMA) * student_new

    wide = tokens.astype(jnp.float32)
    normed = (
        wide * lax.rsqrt(jnp.mean(wide * wide, axis=-1, keepdims=True) + 1e-06) * norm_gain
    ).astype(jnp.bfloat16)
    other = lax.ppermute(normed, "core", swap)

    for s in range(4):
        for k in range(COLORS):
            got = exchange(copied[k], DIMS[k][s // 2], (FIRST, SECOND)[s % 2])
            copied[k] = jnp.concatenate([copied[k], got], axis=0)
    gains = jnp.stack([query_gain, key_gain])
    units, begun = [], []
    for k in range(COLORS):
        one = exchange(copied[k], DIMS[k][2], FIRST)
        two = exchange(copied[k], DIMS[k][2], SECOND)
        three = exchange(one, DIMS[k][2], SECOND)
        units.append([copied[k], one, two, three])
        begun += project_half(k, 0, where, normed, other, gains, [copied[k], one, two, copied[k]])
    outputs, back = (), []
    for k in (1, 2, 0):
        *outputs, send = project_half(k, 1, where, normed, other, gains, units[k], begun[k], outputs)
        back.append(lax.ppermute(send, "core", swap))
    where, student_new, teacher_new = lax.optimization_barrier((where, student_new, teacher_new))
    outputs = put(1, where, back[:2], *outputs)
    outputs = put(0, where, back[2:], *outputs)
    return (teacher_new, student_new, *outputs)


def solution(mesh):
    split = Mesh(np.asarray(mesh.devices).reshape(2, 2, 4, 4, 2), ("zlo", "core", "y", "x", "zhi"))
    group, fsdp = ("zlo", "core"), ("y", "x", "zhi")
    rows = P(group + fsdp, None)

    return jax.shard_map(
        shards,
        mesh=split,
        in_specs=(rows, P(group, fsdp, None), P(fsdp, group), P(), P(), P()),
        out_specs=(P(fsdp, group), P(fsdp, group), rows, rows),
        check_vma=False,
    )
```

```python
import jax
import jax.numpy as jnp
import numpy as np
from jax import lax
from jax.experimental import pallas as pl
from jax.experimental.pallas import tpu as pltpu
from jax.sharding import Mesh
from jax.sharding import PartitionSpec as P

HEAD = 128
EMA = 0.99
COLORS = 3
VMEM_LIMIT = 20 * 2**20
TILE = 256
FIRST, SECOND = (1, 3), (3, 1)
ORDER = (180, 156)
DIMS = (("x", "y", "z"), ("y", "z", "x"), ("z", "x", "y"))


def exchange(x, dim, masks):
    if dim == "z":
        axes = ("zlo", "core", "zhi")
        pairs = []
        for zlo in range(2):
            for core in range(2):
                for zhi in range(2):
                    z = (2 * zhi + zlo) ^ masks[core]
                    pairs.append(((zlo * 2 + core) * 2 + zhi, ((z % 2) * 2 + core) * 2 + z // 2))
    else:
        axes = ("core", dim)
        pairs = [(core * 4 + i, core * 4 + (i ^ masks[core])) for core in range(2) for i in range(4)]
    return lax.ppermute(x, axes, pairs)


def fill(color, half, units, held, n):
    core = lax.axis_index("core")
    order = ORDER[0] + (ORDER[1] - ORDER[0]) * core
    dims = DIMS[color]
    place = {
        "x": lax.axis_index("x"),
        "y": lax.axis_index("y"),
        "z": 2 * lax.axis_index("zhi") + lax.axis_index("zlo"),
    }
    seen = {d: [lax.bitwise_xor(v, lax.bitwise_and(lax.shift_right_logical(order, 2 * i), 3)) for i in range(4)] for d, v in place.items()}
    low = lambda v: lax.bitwise_and(v, 1)
    high = lambda v: lax.shift_right_logical(v, 1)
    rows = units[0].shape[1]
    if dims[2] == "z":
        row_of = {"x": lambda v: v * 2, "y": lambda v: v * 8, "z": high}
    elif dims[2] == "x":
        row_of = {"x": lambda v: low(v) * 2, "y": lambda v: v * 4, "z": high}
    else:
        row_of = {"x": lambda v: v * 2, "y": lambda v: low(v) * 8, "z": high}
    at_row = {d: [row_of[d](v) * rows for v in seen[d]] for d in dims}
    at_col = [0 if dims[2] == "z" else low(v) * n for v in seen["z"]]

    def copy(u):
        for pos in range(16):
            i = dict(zip(dims, (pos % 4, pos // 4, u)))
            row = pl.multiple_of(at_row["x"][i["x"]] + at_row["y"][i["y"]] + at_row["z"][i["z"]], rows)
            col = at_col[i["z"]]
            col = col if isinstance(col, int) else pl.multiple_of(col, n)
            held[pl.ds(row, rows), pl.ds(col, n)] = units[u][pos]

    if dims[2] == "z":
        for u in ((1, 2), (0, 3))[half]:
            copy(u)
    else:
        copy((0, 3)[half])
        for u in (1, 2):
            pl.when(core == (u - 1 if half == 0 else 2 - u))(lambda u=u: copy(u))


def tokens_of(color, half, src, m):
    last = DIMS[color][2]
    span = slice(m, m + TILE)
    if last == "z":
        return src[span, :]
    width = src.shape[1]
    side = lax.bitwise_xor(lax.shift_right_logical(lax.axis_index(last), 1), half)
    if last == "y":
        return src[span, pl.ds(pl.multiple_of(side * (width // 2), HEAD), width // 2)]
    cut = width // 8
    return jnp.concatenate(
        [src[span, pl.ds(pl.multiple_of(side * cut + y * 2 * cut, HEAD), cut)] for y in range(4)], axis=1
    )


def head_norm(v, gain):
    v = v * lax.rsqrt(jnp.mean(v * v, axis=-1, keepdims=True) + 1e-06) * gain
    return v.astype(jnp.bfloat16)


def begin_body(color, where, own, other, gains, *refs):
    units, (out, held) = refs[:4], refs[4:]
    n = units[0].shape[2]
    fill(color, 0, units, held, n)
    for t, src in enumerate((own, other)):
        for m in range(0, own.shape[0], TILE):
            y = jnp.dot(tokens_of(color, 0, src, m), held[...], preferred_element_type=jnp.float32)
            if DIMS[color][2] == "z":
                y = y * own.shape[1] ** (-0.5)
                gain = jnp.where(where[1] == 0, gains[1:2, :], gains[0:1, :])
                for h in range(0, n, HEAD):
                    out[t, m : m + TILE, h : h + HEAD] = head_norm(y[:, h : h + HEAD], gain)
            else:
                out[t, m : m + TILE, :] = y


def end_body(color, n_held, where, own, other, gains, begun, *refs):
    units = refs[:4]
    q_out, k_out, send_out, held = refs[4 + n_held :]
    n = units[0].shape[2]
    scale = own.shape[1] ** (-0.5)
    fill(color, 1, units, held, n)
    for t, src in enumerate((own, other)):
        for m in range(0, own.shape[0], TILE):
            span = slice(m, m + TILE)
            y = jnp.dot(tokens_of(color, 1, src, m), held[...], preferred_element_type=jnp.float32)
            outs = (q_out, k_out) if t == 0 else (send_out.at[0], send_out.at[1])
            if DIMS[color][2] == "z":
                y = y * scale
                gain = jnp.where(where[1] == 0, gains[0:1, :], gains[1:2, :])
                mine = jnp.concatenate([head_norm(y[:, h : h + HEAD], gain) for h in range(0, n, HEAD)], axis=1)
                early = begun[t, span, :]
                for i, out in enumerate(outs):
                    out[span, :] = jnp.where(where[1] == i, mine, early)
            else:
                y = (y + begun[t, span, :]) * scale
                for i, out in enumerate(outs):
                    for h in range(0, n, HEAD):
                        out[span, h : h + HEAD] = head_norm(y[:, i * n + h : i * n + h + HEAD], gains[i : i + 1, :])


def project_half(color, half, where, own, other, gains, units, begun=None, outputs=()):
    tokens, width = own.shape
    n = units[0].shape[2]
    vmem, any_spec = pl.BlockSpec(memory_space=pltpu.VMEM), pl.BlockSpec(memory_space=pl.ANY)
    operands = [own, other, gains, *([] if half == 0 else [begun]), *units, *outputs]
    specs = [vmem] * (len(operands) - len(outputs)) + [any_spec] * len(outputs)
    by_block = DIMS[color][2] == "z"
    whole = lambda *shape: pl.BlockSpec(shape, lambda i, *_: (0,) * len(shape))
    if half == 0:
        body = lambda *refs: begin_body(color, *refs)
        out_shape = [jax.ShapeDtypeStruct((2, tokens, n), jnp.bfloat16) if by_block else jax.ShapeDtypeStruct((2, tokens, 2 * n), jnp.float32)]
        out_specs = [vmem]
        aliases = {}
    else:
        body = lambda *refs: end_body(color, len(outputs), *refs)
        big = jax.ShapeDtypeStruct((tokens, width), jnp.bfloat16)
        out_shape = [big, big, jax.ShapeDtypeStruct((2, tokens, n), jnp.bfloat16)]
        col = lambda i, where: (0, where[0] * COLORS + color)
        out_specs = [pl.BlockSpec((tokens, n), col), pl.BlockSpec((tokens, n), col), whole(2, tokens, n)]
        first = 1 + len(operands) - len(outputs)
        aliases = {first: 0, first + 1: 1} if outputs else {}
    return pl.pallas_call(
        body,
        grid_spec=pltpu.PrefetchScalarGridSpec(
            num_scalar_prefetch=1,
            grid=(1,),
            in_specs=specs,
            out_specs=out_specs,
            scratch_shapes=[pltpu.VMEM((width, n) if by_block else (width // 2, 2 * n), jnp.bfloat16)],
        ),
        out_shape=out_shape,
        input_output_aliases=aliases,
        compiler_params=pltpu.CompilerParams(vmem_limit_bytes=VMEM_LIMIT),
        cost_estimate=pl.CostEstimate(
            flops=2 * 2 * tokens * width * n,
            bytes_accessed=2 * width * (2 * tokens + 2 * n),
            transcendentals=0,
        ),
    )(where, *operands)


def put_body(n_got, where, *refs):
    q_out, k_out = refs[n_got + 2 :]
    for i in range(n_got):

        @pl.when(pl.program_id(0) == i)
        def _():
            q_out[...] = refs[i][0]
            k_out[...] = refs[i][1]


def put(color, where, got, query, key_out):
    _, half, n = got[0].shape
    col = lambda i, where: (0, (1 - where[0]) * COLORS + color + i)
    any_spec = pl.BlockSpec(memory_space=pl.ANY)
    return pl.pallas_call(
        lambda *refs: put_body(len(got), *refs),
        grid_spec=pltpu.PrefetchScalarGridSpec(
            num_scalar_prefetch=1,
            grid=(len(got),),
            in_specs=[pl.BlockSpec((2, half, n), lambda *_: (0, 0, 0))] * len(got) + [any_spec, any_spec],
            out_specs=[pl.BlockSpec((half, n), col)] * 2,
        ),
        out_shape=[jax.ShapeDtypeStruct(query.shape, query.dtype)] * 2,
        input_output_aliases={1 + len(got): 0, 2 + len(got): 1},
        compiler_params=pltpu.CompilerParams(vmem_limit_bytes=12 * 2**20),
        cost_estimate=pl.CostEstimate(flops=10**9, bytes_accessed=8 * len(got) * got[0].size, transcendentals=0),
    )(where, *got, query, key_out)


def pick_body(core, local, out):
    out[0] = local[...]


def pick(core, local, block):
    rows = local.shape[0]
    return pl.pallas_call(
        pick_body,
        grid_spec=pltpu.PrefetchScalarGridSpec(
            num_scalar_prefetch=1,
            grid=(2,),
            in_specs=[pl.BlockSpec((rows, block), lambda j, core: (0, 2 * j + 1 - core[0]))],
            out_specs=pl.BlockSpec((1, rows, block), lambda j, core: (j, 0, 0)),
        ),
        out_shape=jax.ShapeDtypeStruct((2, rows, block), jnp.float32),
        compiler_params=pltpu.CompilerParams(vmem_limit_bytes=8 * 2**20),
        cost_estimate=pl.CostEstimate(flops=10**9, bytes_accessed=16 * rows * block, transcendentals=0),
        name="pick",
    )(core, local)


def merge_body(n, where, local, got, keep, rest, *give):
    total = local[...] + got[0]
    mine = pl.program_id(0) == where[1]

    @pl.when(mine)
    def _():
        keep[...] = total

    @pl.when(jnp.logical_not(mine))
    def _():
        high = total.astype(jnp.bfloat16)
        rest[...] = (total - high.astype(jnp.float32)).astype(jnp.bfloat16)
        for k in range(COLORS):
            give[k][...] = high[:, k * n : (k + 1) * n]


def merge(where, local, got):
    _, rows, block = got.shape
    n = block // COLORS
    return pl.pallas_call(
        lambda *refs: merge_body(n, *refs),
        grid_spec=pltpu.PrefetchScalarGridSpec(
            num_scalar_prefetch=1,
            grid=(2,),
            in_specs=[
                pl.BlockSpec((rows, block), lambda j, where: (0, 2 * j + where[0])),
                pl.BlockSpec((1, rows, block), lambda j, where: (j, 0, 0)),
            ],
            out_specs=[pl.BlockSpec((rows, block), lambda *_: (0, 0))] * 2 + [pl.BlockSpec((rows, n), lambda *_: (0, 0))] * COLORS,
        ),
        out_shape=[jax.ShapeDtypeStruct((rows, block), jnp.float32), jax.ShapeDtypeStruct((rows, block), jnp.bfloat16)]
        + [jax.ShapeDtypeStruct((rows, n), jnp.bfloat16)] * COLORS,
        compiler_params=pltpu.CompilerParams(vmem_limit_bytes=16 * 2**20),
        cost_estimate=pl.CostEstimate(flops=10**9, bytes_accessed=24 * rows * block, transcendentals=0),
        name="merge",
    )(where, local, got)


def shards(tokens, student, teacher, norm_gain, query_gain, key_gain):
    block = teacher.shape[1]
    n = block // COLORS
    core = lax.axis_index("core")
    where = jnp.stack([core, lax.axis_index("zlo")]).astype(jnp.int32)
    swap = [(0, 1), (1, 0)]

    local = student[0]
    got = lax.ppermute(pick(where, local, block), "core", swap)
    keep, rest, *give = merge(where, local, got)
    arrived, copied = [], []
    for k in range(COLORS):
        arrived.append(lax.ppermute(give[k], "zlo", swap).astype(jnp.float32))
    rest = lax.ppermute(rest, "zlo", swap).astype(jnp.float32)
    for k in range(COLORS):
        cut = keep[:, k * n : (k + 1) * n]
        if k:
            cut, _ = lax.optimization_barrier((cut, copied[-1]))
        copied.append(((cut + arrived[k]) / 4).astype(jnp.bfloat16)[None])
    high = jnp.concatenate(arrived, axis=1)
    student_new = (keep + (high + rest)) / 4
    teacher_new = EMA * teacher + (1.0 - EMA) * student_new

    wide = tokens.astype(jnp.float32)
    normed = (
        wide * lax.rsqrt(jnp.mean(wide * wide, axis=-1, keepdims=True) + 1e-06) * norm_gain
    ).astype(jnp.bfloat16)
    other = lax.ppermute(normed, "core", swap)

    for s in range(4):
        for k in range(COLORS):
            got = exchange(copied[k], DIMS[k][s // 2], (FIRST, SECOND)[s % 2])
            copied[k] = jnp.concatenate([copied[k], got], axis=0)
    gains = jnp.stack([query_gain, key_gain])
    units, begun = [], []
    for k in range(COLORS):
        one = exchange(copied[k], DIMS[k][2], FIRST)
        two = exchange(copied[k], DIMS[k][2], SECOND)
        three = exchange(one, DIMS[k][2], SECOND)
        units.append([copied[k], one, two, three])
        begun += project_half(k, 0, where, normed, other, gains, [copied[k], one, two, copied[k]])
    outputs, back = (), []
    where, student_new, teacher_new = lax.optimization_barrier((where, student_new, teacher_new))
    for k in range(COLORS):
        *outputs, send = project_half(k, 1, where, normed, other, gains, units[k], begun[k], outputs)
        back.append(lax.ppermute(send, "core", swap))
    outputs = put(0, where, back[:2], *outputs)
    outputs = put(2, where, back[2:], *outputs)
    return (teacher_new, student_new, *outputs)


def solution(mesh):
    split = Mesh(np.asarray(mesh.devices).reshape(2, 2, 4, 4, 2), ("zlo", "core", "y", "x", "zhi"))
    group, fsdp = ("zlo", "core"), ("y", "x", "zhi")
    rows = P(group + fsdp, None)

    return jax.shard_map(
        shards,
        mesh=split,
        in_specs=(rows, P(group, fsdp, None), P(fsdp, group), P(), P(), P()),
        out_specs=(P(fsdp, group), P(fsdp, group), rows, rows),
        check_vma=False,
    )
```
